128 devices in a mesh: pts: 64 (over z, y, x), rows: 2 (over core).
Axes of the slice: x: 4, y: 4, z: 4, core: 2. Of those that a mesh axis runs over, the one named last changes fastest.
Arguments:
- vertex: bfloat16 [64, 960, 960], P('pts', 'rows'), may hold values from -0.1875 to 0.1875
- bubble: float32 [64, 960], P('pts'), may hold values from -2 to -0.2
- cross_deriv: bfloat16 [64, 960, 960], P('pts', 'rows'), may hold values from -6 to 6
- send_blocks: int32 [64, 64, 2], P('pts'), may hold values from -1 to 14, as said below
- recv_slots: int32 [64, 15], P('pts'), may hold values from 0 to 127, as said below
- freq_shift: int32 [64, 15], P('pts'), may hold values from -16 to 16
- proj_coef: float32 [64, 15], P('pts'), may hold values from -1.5 to 1.5
Outputs:
- left_insertion: bfloat16 [64, 960, 960], P('pts', 'rows')
The draws below stay inside these ranges and needn't reach their ends.
Inputs may be any that keep to these rules, and one draw needn't show every extreme that they name: `send_blocks`: entry [d, e, c] is -1 for an empty slot, else the index p * 15 + g of the box (local point p, form factor g) of device d along pts that fills slot c towards device e. For every e some d fills all 2 slots towards e. `recv_slots`: entry [q, f] is 2 * d + c for a slot c towards device q // 1 along pts whose send_blocks entry [d, q, c] is not -1; each such slot is named by exactly one entry of that device's points.
All inputs are finite; a program needn't handle non-finite values.
Results may differ from the reference program's by a relative error of at most 0.0058.
Values may be sent and summed in bfloat16 or wider, within the bound.
A program may use at most 128 MiB of HBM per device.

```python
import jax
import jax.numpy as jnp
from jax import lax

NFF = 15
NFREQ = 64
ORDER = 960
PT_DEV = 1
POINTS = 64
CAP = 2
N_PTS = 64


def routing(key):
    possible_targets = N_PTS * CAP
    wanted_count = PT_DEV * NFF
    extra_weight_each_processor = jax.random.randint(jax.random.fold_in(key, 1), (N_PTS,), 0, 3)
    hot_dev = jax.random.randint(jax.random.fold_in(key, 2), (N_PTS,), 0, N_PTS)
    sorted_positions = jax.vmap(lambda k: jax.random.permutation(k, possible_targets))(jax.random.split(jax.random.fold_in(key, 3), N_PTS))
    possible_processor = jnp.arange(possible_targets, dtype=jnp.int32) // CAP
    heavy_marker = (possible_processor[None, :] == hot_dev[:, None]).astype(jnp.int32)
    rating_numbers = sorted_positions.astype(jnp.int32) + possible_targets * (extra_weight_each_processor[possible_processor][None, :] + 3 * heavy_marker)
    unused, chosen = lax.top_k(rating_numbers, wanted_count)
    mixing = jax.vmap(lambda k: jax.random.permutation(k, wanted_count))(jax.random.split(jax.random.fold_in(key, 4), N_PTS))
    chosen = jnp.take_along_axis(chosen, mixing, axis=1).astype(jnp.int32)
    block_ids = jax.random.randint(jax.random.fold_in(key, 5), (N_PTS, wanted_count), 0, wanted_count)
    rows_dest = jnp.broadcast_to(jnp.arange(N_PTS, dtype=jnp.int32)[:, None], (N_PTS, wanted_count))
    table = jnp.full((N_PTS, possible_targets), -1, jnp.int32).at[rows_dest, chosen].set(block_ids.astype(jnp.int32))
    outbound_routing_grid = table.reshape(N_PTS, N_PTS, CAP).transpose(1, 0, 2)
    recv_table = chosen.reshape(N_PTS * PT_DEV, NFF)
    return (outbound_routing_grid, recv_table)


def draw_send_blocks(key, part):
    return routing(jax.random.fold_in(key, 7))[0]


def draw_recv_slots(key, part):
    return routing(jax.random.fold_in(key, 7))[1]


def set_ends(array, stream_key, smallest, top_value):
    longest = array.shape.index(max(array.shape))
    spots = []
    for shift in (0, 1):
        where = [jax.random.randint(jax.random.fold_in(stream_key, axis), (), 0, length) for axis, length in enumerate(array.shape)]
        where[longest] = (where[longest] + shift) % array.shape[longest]
        spots.append(tuple(where))
    return array.at[spots[0]].set(smallest).at[spots[1]].set(top_value)


def block_levels(key, shape, cuts, least, high):
    level, own = 1.0, jax.random.fold_in(key, 6)
    for position, shards_of in cuts:
        draws = jnp.exp(jax.random.uniform(jax.random.fold_in(own, position), (shards_of,), jnp.float32, least / len(cuts), high / len(cuts)))
        level = level * jnp.repeat(draws, shape[position] // shards_of).reshape([-1 if axis == position else 1 for axis in range(len(shape))])
    return level


def gaussian(rng, dims, width, limit, shards=(), kind=jnp.bfloat16):
    loudness = block_levels(rng, dims, shards, -0.22, 0.18) if shards else 1.0
    array = jax.random.normal(rng, dims, jnp.float32) * width * loudness
    return jnp.minimum(jnp.maximum(array, -limit), limit).astype(kind)


def setup_inputs(seed: int = 0) -> dict:
    key_list = jax.random.split(jax.random.key(seed), 8)
    return {
        "vertex": gaussian(key_list[0], (POINTS, ORDER, ORDER), ORDER ** -0.5, 0.1875, ((0, 64), (1, 2))),
        "bubble": jnp.clip(-2.0 + 1.8 * jax.random.uniform(key_list[1], (POINTS, ORDER), jnp.float32) ** block_levels(key_list[1], (POINTS, ORDER), ((0, 64),), -0.2, 0.2), -2.0, -0.2),
        "cross_deriv": gaussian(key_list[2], (POINTS, ORDER, ORDER), 1.0, 6.0, ((0, 64), (1, 2))),
        "send_blocks": draw_send_blocks(jax.random.fold_in(key_list[7], 71), 0),
        "recv_slots": draw_recv_slots(jax.random.fold_in(key_list[7], 71), 0),
        "freq_shift": set_ends(jax.random.randint(key_list[5], (POINTS, NFF), 0 - NFREQ // 4, NFREQ // 4 + 1), jax.random.fold_in(key_list[5], 1), 0 - NFREQ // 4, (NFREQ // 4 + 1) - 1).astype(jnp.int32),
        "proj_coef": jnp.clip(jax.random.uniform(key_list[6], (POINTS, NFF), jnp.float32, -1.5, 1.5) * block_levels(key_list[6], (POINTS, NFF), ((0, 64),), -0.4, 0.0), -1.5, 1.5),
    }


def reference(vertex, bubble, cross_deriv, send_blocks, recv_slots, freq_shift, proj_coef):
    freq_grid = jnp.arange(NFREQ, dtype=jnp.int32)

    def take_box(src_point, src_form, shift_by, weight_of):
        stripe = lax.dynamic_slice(cross_deriv, (src_point, jnp.int32(0), src_form * NFREQ), (1, ORDER, NFREQ))[0]
        source_freq = freq_grid + shift_by
        inside = (source_freq >= 0) & (source_freq < NFREQ)
        shifted = jnp.take(stripe, jnp.clip(source_freq, 0, NFREQ - 1), axis=1)
        return jnp.where(inside[None, :], shifted.astype(jnp.float32) * weight_of, 0.0)

    def one_point(packed):
        point_idx, vertex_pt, bubble_pt, slot_row, shift_row, coef_row = packed
        owner_dev = point_idx // PT_DEV
        source_dev = slot_row // CAP
        block_idx = send_blocks[source_dev, owner_dev, slot_row % CAP]
        src_points = (source_dev * PT_DEV + block_idx // NFF).astype(jnp.int32)
        source_form_list = (block_idx % NFF).astype(jnp.int32)
        box_values = jax.vmap(take_box)(src_points, source_form_list, shift_row, coef_row)
        remapped = box_values.transpose(1, 0, 2).reshape(ORDER, ORDER).astype(jnp.bfloat16)
        scaled = (vertex_pt.astype(jnp.float32) * bubble_pt[None, :]).astype(jnp.bfloat16)
        return jnp.dot(scaled, remapped, preferred_element_type=jnp.float32).astype(jnp.bfloat16)

    return lax.map(one_point, (jnp.arange(POINTS, dtype=jnp.int32), vertex, bubble, recv_slots, freq_shift, proj_coef))
```

```python
import jax
import jax.numpy as jnp
from jax import lax
from jax.sharding import PartitionSpec as P

SLOTS = 16


def exchange(array, axis):
    return lax.all_to_all(array, axis, split_axis=0, concat_axis=0, tiled=True)


def body(vertex, bubble, cross_deriv, send_blocks, recv_slots, freq_shift, proj_coef):
    _, rows, width = vertex.shape
    forms = recv_slots.shape[1]
    freqs = width // forms
    points = send_blocks.shape[1]
    cap = send_blocks.shape[2]
    f32, bf16 = jnp.float32, jnp.bfloat16

    boxes = cross_deriv[0].reshape(rows, forms, freqs).transpose(2, 1, 0)
    table = jnp.concatenate([send_blocks[0].T.reshape(-1), recv_slots[0]]).astype(bf16)
    table = jnp.pad(table, (0, rows - table.shape[0]))
    table = jnp.broadcast_to(table[None, None], (freqs, 1, rows))
    got = exchange(jnp.concatenate([boxes, table], axis=1), "pts")

    tables = got[:, forms, :]
    sb = tables[:, : cap * points].astype(f32).reshape(points, cap, points)
    rs = tables[:, cap * points : cap * points + forms].astype(f32)
    rs = jnp.pad(rs, ((0, 0), (0, SLOTS - forms)), constant_values=-1.0)
    source = jnp.arange(points * SLOTS, dtype=jnp.int32)
    src_dev = (source // SLOTS).astype(f32)
    src_form = (source % SLOTS).astype(f32)
    pick = jnp.zeros((points, SLOTS, points * SLOTS), jnp.bool_)
    for c in range(cap):
        held = jnp.repeat(sb[:, c, :].T, SLOTS, axis=1)
        slot = jnp.where(held == src_form[None], src_dev[None] * cap + c, -2.0)
        pick = pick | (rs[:, :, None] == slot[:, None, :])
    pick = pick.astype(bf16).reshape(points * SLOTS, points * SLOTS)
    chosen = jnp.dot(pick, got.reshape(points * SLOTS, rows), preferred_element_type=f32)
    chosen = chosen.astype(bf16).reshape(points, SLOTS, rows)
    mine = exchange(chosen, "pts").reshape(freqs * SLOTS, rows)

    line = jnp.arange(freqs * SLOTS, dtype=jnp.int32)
    column = jnp.arange(width, dtype=jnp.int32)
    wanted_n = column % freqs + jnp.repeat(freq_shift[0], freqs)
    wanted = jnp.where(
        (wanted_n >= 0) & (wanted_n < freqs), wanted_n * SLOTS + column // freqs, -1
    )
    shift = (line[:, None] == wanted[None, :]).astype(bf16)
    moved = lax.dot_general(mine, shift, (((0,), (0,)), ((), ())), preferred_element_type=f32)
    remapped = (moved * jnp.repeat(proj_coef[0], freqs)[None]).astype(bf16)
    both = exchange(jnp.broadcast_to(remapped, (2, rows, width)), "rows").reshape(2 * rows, width)
    scaled = (vertex[0].astype(f32) * bubble[0][None]).astype(bf16)
    out = jnp.dot(scaled, both, preferred_element_type=f32)
    return out.astype(bf16)[None]


def solution(mesh):
    in_specs = (
        P("pts", "rows", None),
        P("pts", None),
        P("pts", "rows", None),
        P("pts", None, None),
        P("pts", None),
        P("pts", None),
        P("pts", None),
    )
    out_specs = P("pts", "rows", None)
    return jax.shard_map(body, mesh=mesh, in_specs=in_specs, out_specs=out_specs, check_vma=False)
```

```python
import functools

import jax
import jax.numpy as jnp
from jax import lax
from jax.experimental import pallas as pl
from jax.experimental.pallas import tpu as pltpu
from jax.sharding import PartitionSpec as P

MESH = pl.DeviceIdType.MESH
F32, BF16, I32 = jnp.float32, jnp.bfloat16, jnp.int32
FORMS, FREQS, POINTS, SIDE = 15, 64, 64, 4
LINES = 16
WIDTH = FORMS * FREQS
ROWS = WIDTH // 2
SLICES = ((0, 256), (256, 224))
PART = 256


def hops(delta):
    return sum(min(d, SIDE - d) for d in delta)


DELTAS = sorted(
    ((a, b, c) for a in range(SIDE) for b in range(SIDE) for c in range(SIDE) if (a, b, c) != (0, 0, 0)),
    key=lambda d: (-hops(d), (d[0] * 5 + d[1] * 11 + d[2] * 23) % 16),
)


def iota(shape, dim):
    return lax.broadcasted_iota(I32, shape, dim)


def remap_kernel(
    x_hbm, sb_ref, rs_ref, shift_ref, coef_ref, o_ref,
    x_ref, perm_ref, table_ref, ta, ra, ub, rb, pick_ref, shift_mat,
    load_sem, send_a, recv_a, send_b, recv_b, send_c, recv_c,
):
    me = lax.axis_index("pts")
    row = lax.axis_index("rows")
    mz, my, mx = me // (SIDE * SIDE), (me // SIDE) % SIDE, me % SIDE

    def peer(delta):
        dz, dy, dx = delta
        return (((mz + dz) % SIDE) * SIDE + (my + dy) % SIDE) * SIDE + (mx + dx) % SIDE

    barrier = pltpu.get_barrier_semaphore()
    for delta in DELTAS:
        pl.semaphore_signal(barrier, inc=1, device_id={"pts": peer(delta)}, device_id_type=MESH)
    pl.semaphore_signal(barrier, inc=1, device_id={"rows": 1 - row}, device_id_type=MESH)

    load = pltpu.make_async_copy(x_hbm, x_ref.at[pl.ds(0, ROWS)], load_sem)
    load.start()

    def build_perm(i, _):
        base = pl.multiple_of(i * 128, 128)
        line = iota((128, WIDTH), 0) + base
        want = jnp.where(line % LINES < FORMS, (line % LINES) * FREQS + line // LINES, -1)
        perm_ref[pl.ds(base, 128), :] = jnp.where(want == iota((128, WIDTH), 1), 1.0, 0.0).astype(BF16)
        return 0

    lax.fori_loop(0, FREQS * LINES // 128, build_perm, 0)
    table_ref[...] = jnp.zeros_like(table_ref)
    table_ref[0:1, 0:POINTS] = sb_ref[0:1, :].astype(F32)
    table_ref[0:1, POINTS : POINTS + FORMS] = rs_ref[...].astype(F32)
    table_ref[0:1, 128 : 128 + POINTS] = sb_ref[1:2, :].astype(F32)
    x_ref[ROWS:, :] = jnp.zeros((2 * PART - ROWS, WIDTH), BF16)
    load.wait()
    for s in range(2):
        block = lax.dot_general(
            perm_ref[...], x_ref[s * PART : (s + 1) * PART, :], (((1,), (1,)), ((), ())),
            preferred_element_type=F32,
        ).reshape(FREQS, LINES, PART)
        if s == 0:
            is_table = iota((FREQS, LINES, PART), 1) == FORMS
            block = jnp.where(is_table, table_ref[0:1, :].reshape(1, 1, PART), block)
        ta[s] = block.astype(BF16)
    pl.semaphore_wait(barrier, len(DELTAS) + 1)

    def copy_to(src, dst, send, recv, s, p):
        return pltpu.make_async_remote_copy(
            src_ref=src.at[s, p], dst_ref=dst.at[s, me], send_sem=send.at[s], recv_sem=recv.at[s],
            device_id={"pts": p}, device_id_type=MESH,
        )

    def send_all(src, dst, send, recv, s):
        for delta in DELTAS:
            copy_to(src, dst, send, recv, s, peer(delta)).start()
        dst[s, me] = src[s, me]

    def all_of(src, dst, send, recv, s):
        n = len(DELTAS)
        return pltpu.make_async_remote_copy(
            src_ref=src.at[s, pl.ds(0, n)], dst_ref=dst.at[s, pl.ds(0, n)], send_sem=send.at[s],
            recv_sem=recv.at[s], device_id={"pts": peer(DELTAS[0])}, device_id_type=MESH,
        )

    for s in range(2):
        send_all(ta, ra, send_a, recv_a, s)

    lane = iota((1, WIDTH), 1)
    moved_by = jnp.zeros((1, WIDTH), I32)
    weight = jnp.zeros((1, WIDTH), F32)
    for f in range(FORMS):
        here = lane // FREQS == f
        moved_by = jnp.where(here, shift_ref[0, f], moved_by)
        weight = jnp.where(here, coef_ref[0, f], weight)
    wanted_n = lane % FREQS + moved_by
    wanted = jnp.where((wanted_n >= 0) & (wanted_n < FREQS), wanted_n * LINES + lane // FREQS, -1)

    def build_shift(i, _):
        base = pl.multiple_of(i * 128, 128)
        line = iota((128, WIDTH), 0) + base
        shift_mat[pl.ds(base, 128), :] = jnp.where(line == wanted, 1.0, 0.0).astype(BF16)
        return 0

    lax.fori_loop(0, FREQS * LINES // 128, build_shift, 0)

    total = POINTS * LINES
    source = iota((POINTS, total), 1)
    widen = jnp.where(iota((POINTS, total), 0) == source // LINES, 1.0, 0.0).astype(BF16)
    form_of = (source % LINES).astype(F32)
    slot_of = (source // LINES * 2).astype(F32)

    for s in range(2):
        all_of(ta, ra, send_a, recv_a, s).wait_recv()
        if s == 0:
            tables = ra[0, :, FORMS, :].astype(F32)
            slots = []
            for c in range(2):
                held = lax.dot_general(
                    tables[:, c * 128 : c * 128 + 128].astype(BF16), widen, (((0,), (0,)), ((), ())),
                    preferred_element_type=F32,
                )[:POINTS]
                slots.append(jnp.where(held == form_of, slot_of + c, -7.0))
            table_ref[pl.ds(0, POINTS), 0:128] = tables[:, 0:128]
            for q in range(0, POINTS, 8):
                named = jnp.broadcast_to(
                    table_ref[q : q + 8, 0:128].reshape(8, 1, 128), (8, LINES, 128)
                ).reshape(8 * LINES, 128)
                f = iota((8 * LINES, 128), 0) % LINES
                at = iota((8 * LINES, 128), 1)
                named = jnp.sum(jnp.where(at == POINTS + f, named, 0.0), axis=1, keepdims=True)
                named = jnp.where(f[:, 0:1] == FORMS, -1.0, named)
                hit = None
                for c in range(2):
                    slot = jnp.broadcast_to(
                        slots[c][q : q + 8].reshape(8, 1, total), (8, LINES, total)
                    ).reshape(8 * LINES, total)
                    hit = (named == slot) if hit is None else hit | (named == slot)
                pick_ref[q * LINES : (q + 8) * LINES, :] = jnp.where(hit, 1.0, 0.0).astype(BF16)
        chosen = jnp.dot(
            pick_ref[...], ra[s].reshape(total, PART), preferred_element_type=F32
        )
        ub[s] = chosen.astype(BF16).reshape(POINTS, LINES, PART)
        send_all(ub, rb, send_b, recv_b, s)

    swaps = []
    for s, (first, size) in enumerate(SLICES):
        all_of(ub, rb, send_b, recv_b, s).wait_recv()
        moved = lax.dot_general(
            rb[s].reshape(FREQS * LINES, PART), shift_mat[...], (((0,), (0,)), ((), ())),
            preferred_element_type=F32,
        )
        where = o_ref.at[pl.ds(pl.multiple_of(row * ROWS + first, 32), size)]
        where[...] = (moved * weight).astype(BF16)[:size]
        swap = pltpu.make_async_remote_copy(
            src_ref=where, dst_ref=where, send_sem=send_c.at[s], recv_sem=recv_c.at[s],
            device_id={"rows": 1 - row}, device_id_type=MESH,
        )
        swap.start()
        swaps.append(swap)
    for s in range(2):
        all_of(ta, ra, send_a, recv_a, s).wait_send()
        all_of(ub, rb, send_b, recv_b, s).wait_send()
        swaps[s].wait()


def remap(x, sb, rs, shift, coef):
    vmem = pl.BlockSpec(memory_space=pltpu.VMEM)
    smem = pl.BlockSpec(memory_space=pltpu.SMEM)
    boxes = pltpu.VMEM((2, POINTS, LINES, PART), BF16)
    total = POINTS * LINES
    pair = pltpu.SemaphoreType.DMA((2,))
    return pl.pallas_call(
        remap_kernel,
        out_shape=jax.ShapeDtypeStruct((WIDTH, WIDTH), BF16),
        in_specs=[pl.BlockSpec(memory_space=pl.ANY), vmem, vmem, smem, smem],
        out_specs=vmem,
        scratch_shapes=[
            pltpu.VMEM((2 * PART, WIDTH), BF16),
            pltpu.VMEM((FREQS * LINES, WIDTH), BF16),
            pltpu.VMEM((POINTS, PART), F32),
            boxes, boxes, boxes, boxes,
            pltpu.VMEM((total, total), BF16),
            pltpu.VMEM((FREQS * LINES, WIDTH), BF16),
            pltpu.SemaphoreType.DMA, pair, pair, pair, pair, pair, pair,
        ],
        compiler_params=pltpu.CompilerParams(
            collective_id=0, has_side_effects=True, vmem_limit_bytes=48 * 1024 * 1024
        ),
        cost_estimate=pl.CostEstimate(flops=10**10, bytes_accessed=10**7, transcendentals=0),
    )(x, sb, rs, shift, coef)


def body(vertex, bubble, cross_deriv, send_blocks, recv_slots, freq_shift, proj_coef):
    remapped = remap(cross_deriv[0], send_blocks[0].T, recv_slots, freq_shift, proj_coef)
    scaled = (vertex[0].astype(F32) * bubble[0][None]).astype(BF16)
    out = jnp.dot(scaled, remapped, preferred_element_type=F32)
    return out.astype(BF16)[None]


def solution(mesh):
    in_specs = (
        P("pts", "rows", None),
        P("pts", None),
        P("pts", "rows", None),
        P("pts", None, None),
        P("pts", None),
        P("pts", None),
        P("pts", None),
    )
    out_specs = P("pts", "rows", None)
    return jax.shard_map(body, mesh=mesh, in_specs=in_specs, out_specs=out_specs, check_vma=False)
```

```python
import functools

import jax
import jax.numpy as jnp
from jax import lax
from jax.experimental import pallas as pl
from jax.experimental.pallas import tpu as pltpu
from jax.sharding import PartitionSpec as P

MESH = pl.DeviceIdType.MESH
F32, BF16, I32 = jnp.float32, jnp.bfloat16, jnp.int32
FORMS, FREQS, POINTS, SIDE = 15, 64, 64, 4
LINES = 16
WIDTH = FORMS * FREQS
ROWS = WIDTH // 2
PART = 256


def hops(delta):
    return sum(min(d, SIDE - d) for d in delta)


DELTAS = sorted(
    ((a, b, c) for a in range(SIDE) for b in range(SIDE) for c in range(SIDE) if (a, b, c) != (0, 0, 0)),
    key=lambda d: (-hops(d), (d[0] * 5 + d[1] * 11 + d[2] * 23) % 16),
)


def iota(shape, dim):
    return lax.broadcasted_iota(I32, shape, dim)


def remap_kernel(
    x_hbm, v_hbm, bub_hbm, sb_hbm, rs_hbm, shift_hbm, coef_hbm, o_ref,
    x_ref, v_ref, bub_ref, sb_ref, rs_ref, shift_ref, coef_ref, perm_ref, table_ref, ta, ra, ub, rb,
    pick_ref, shift_mat, wide_ref, halves, remapped, acc_ref,
    load_sem, send_a, recv_a, send_b, recv_b, send_c, recv_c,
):
    me = lax.axis_index("pts")
    row = lax.axis_index("rows")
    mz, my, mx = me // (SIDE * SIDE), (me // SIDE) % SIDE, me % SIDE

    def peer(delta):
        dz, dy, dx = delta
        return (((mz + dz) % SIDE) * SIDE + (my + dy) % SIDE) * SIDE + (mx + dx) % SIDE

    barrier = pltpu.get_barrier_semaphore()
    for delta in DELTAS:
        pl.semaphore_signal(barrier, inc=1, device_id={"pts": peer(delta)}, device_id_type=MESH)
    pl.semaphore_signal(barrier, inc=1, device_id={"rows": 1 - row}, device_id_type=MESH)

    loads = [
        pltpu.make_async_copy(src, dst, load_sem.at[i])
        for i, (src, dst) in enumerate((
            (x_hbm, x_ref.at[pl.ds(0, ROWS)]), (sb_hbm, sb_ref), (rs_hbm, rs_ref), (shift_hbm, shift_ref),
            (coef_hbm, coef_ref), (bub_hbm, bub_ref), (v_hbm, v_ref),
        ))
    ]
    for load in loads:
        load.start()

    def build_perm(i, _):
        base = pl.multiple_of(i * 128, 128)
        line = iota((128, 1), 0) + base
        g = line & (LINES - 1)
        want = jnp.where(g < FORMS, g * FREQS + (line >> 4), -1)
        perm_ref[pl.ds(base, 128), :] = jnp.where(want == iota((128, WIDTH), 1), 1.0, 0.0).astype(BF16)
        return 0

    lax.fori_loop(0, FREQS * LINES // 128, build_perm, 0)
    table_ref[...] = jnp.zeros_like(table_ref)
    loads[1].wait()
    loads[2].wait()
    table_ref[0:1, 0:POINTS] = sb_ref[0:1, :].astype(F32)
    table_ref[0:1, POINTS : POINTS + FORMS] = rs_ref[...].astype(F32)
    table_ref[0:1, 128 : 128 + POINTS] = sb_ref[1:2, :].astype(F32)
    x_ref[ROWS:, :] = jnp.zeros((2 * PART - ROWS, WIDTH), BF16)
    loads[0].wait()

    def permute(s):
        block = lax.dot_general(
            perm_ref[...], x_ref[s * PART : (s + 1) * PART, :], (((1,), (1,)), ((), ())),
            preferred_element_type=F32,
        ).reshape(FREQS, LINES, PART)
        if s == 0:
            is_table = iota((FREQS, LINES, PART), 1) == FORMS
            block = jnp.where(is_table, table_ref[0:1, :].reshape(1, 1, PART), block)
        ta[s] = block.astype(BF16)

    permute(0)
    pl.semaphore_wait(barrier, len(DELTAS) + 1)

    def copy_to(src, dst, send, recv, s, p):
        return pltpu.make_async_remote_copy(
            src_ref=src.at[s, p], dst_ref=dst.at[s, me], send_sem=send.at[s], recv_sem=recv.at[s],
            device_id={"pts": p}, device_id_type=MESH,
        )

    def send_all(src, dst, send, recv, s):
        for delta in DELTAS:
            copy_to(src, dst, send, recv, s, peer(delta)).start()
        dst[s, me] = src[s, me]

    def all_of(src, dst, send, recv, s):
        n = len(DELTAS)
        return pltpu.make_async_remote_copy(
            src_ref=src.at[s, pl.ds(0, n)], dst_ref=dst.at[s, pl.ds(0, n)], send_sem=send.at[s],
            recv_sem=recv.at[s], device_id={"pts": peer(DELTAS[0])}, device_id_type=MESH,
        )

    send_all(ta, ra, send_a, recv_a, 0)
    permute(1)
    send_all(ta, ra, send_a, recv_a, 1)

    for load in loads[3:]:
        load.wait()
    wide_ref[:, 896:] = jnp.zeros((32, 128), F32)

    def build_halves(i, _):
        at = pl.ds(pl.multiple_of(i * 32, 32), 32)
        scaled = (v_ref[at, :].astype(F32) * bub_ref[...]).astype(BF16).astype(F32)
        wide_ref[:, :WIDTH] = scaled
        inside = iota((32, 2 * PART), 1) < ROWS
        halves[0, at, :] = jnp.where(inside, wide_ref[:, : 2 * PART], 0.0).astype(BF16)
        halves[1, at, :] = pltpu.roll(wide_ref[...], 1024 - ROWS, 1)[:, : 2 * PART].astype(BF16)
        return 0

    lax.fori_loop(0, ROWS // 32, build_halves, 0)
    lane = iota((1, WIDTH), 1)
    moved_by = jnp.zeros((1, WIDTH), I32)
    weight = jnp.zeros((1, WIDTH), F32)
    for f in range(FORMS):
        here = (lane >> 6) == f
        moved_by = jnp.where(here, shift_ref[0, f], moved_by)
        weight = jnp.where(here, coef_ref[0, f], weight)
    wanted_n = (lane & (FREQS - 1)) + moved_by
    wanted = jnp.where((wanted_n >= 0) & (wanted_n < FREQS), wanted_n * LINES + (lane >> 6), -1)

    def build_shift(i, _):
        base = pl.multiple_of(i * 128, 128)
        line = iota((128, WIDTH), 0) + base
        shift_mat[pl.ds(base, 128), :] = jnp.where(line == wanted, 1.0, 0.0).astype(BF16)
        return 0

    lax.fori_loop(0, FREQS * LINES // 128, build_shift, 0)

    total = POINTS * LINES
    source = iota((POINTS, total), 1)
    widen = jnp.where(iota((POINTS, total), 0) == (source >> 4), 1.0, 0.0).astype(BF16)
    form_of = (source & (LINES - 1)).astype(F32)
    slot_of = ((source >> 4) * 2).astype(F32)

    for s in range(2):
        all_of(ta, ra, send_a, recv_a, s).wait_recv()
        if s == 0:
            tables = ra[0, :, FORMS, :].astype(F32)
            slots = []
            for c in range(2):
                held = lax.dot_general(
                    tables[:, c * 128 : c * 128 + 128].astype(BF16), widen, (((0,), (0,)), ((), ())),
                    preferred_element_type=F32,
                )[:POINTS]
                slots.append(jnp.where(held == form_of, slot_of + c, -7.0))
            table_ref[pl.ds(0, POINTS), 0:128] = tables[:, 0:128]
            for q in range(0, POINTS, 8):
                named = jnp.broadcast_to(
                    table_ref[q : q + 8, 0:128].reshape(8, 1, 128), (8, LINES, 128)
                ).reshape(8 * LINES, 128)
                f = iota((8 * LINES, 128), 0) & (LINES - 1)
                at = iota((8 * LINES, 128), 1)
                named = jnp.sum(jnp.where(at == POINTS + f, named, 0.0), axis=1, keepdims=True)
                named = jnp.where(f[:, 0:1] == FORMS, -1.0, named)
                hit = None
                for c in range(2):
                    slot = jnp.broadcast_to(
                        slots[c][q : q + 8].reshape(8, 1, total), (8, LINES, total)
                    ).reshape(8 * LINES, total)
                    hit = (named == slot) if hit is None else hit | (named == slot)
                pick_ref[q * LINES : (q + 8) * LINES, :] = jnp.where(hit, 1.0, 0.0).astype(BF16)
        chosen = jnp.dot(
            pick_ref[...], ra[s].reshape(total, PART), preferred_element_type=F32
        )
        ub[s] = chosen.astype(BF16).reshape(POINTS, LINES, PART)
        send_all(ub, rb, send_b, recv_b, s)

    swaps = []
    for s in range(2):
        all_of(ub, rb, send_b, recv_b, s).wait_recv()
        moved = lax.dot_general(
            rb[s].reshape(FREQS * LINES, PART), shift_mat[...], (((0,), (0,)), ((), ())),
            preferred_element_type=F32,
        )
        remapped[row, s] = (moved * weight).astype(BF16)
        swap = pltpu.make_async_remote_copy(
            src_ref=remapped.at[row, s], dst_ref=remapped.at[row, s], send_sem=send_c.at[s],
            recv_sem=recv_c.at[s], device_id={"rows": 1 - row}, device_id_type=MESH,
        )
        swap.start()
        swaps.append(swap)

        def times(half):
            return jnp.dot(
                halves[half, :, s * PART : (s + 1) * PART], remapped[half, s], preferred_element_type=F32
            )

        if s == 0:
            acc_ref[...] = times(row)
        else:
            acc_ref[...] += times(row)
        swap.wait_recv()
        if s == 0:
            acc_ref[...] += times(1 - row)
        else:
            o_ref[...] = (acc_ref[...] + times(1 - row)).astype(BF16)
    for s in range(2):
        all_of(ta, ra, send_a, recv_a, s).wait_send()
        all_of(ub, rb, send_b, recv_b, s).wait_send()
        swaps[s].wait_send()


def remap(x, vertex, bubble, sb, rs, shift, coef):
    vmem = pl.BlockSpec(memory_space=pltpu.VMEM)
    boxes = pltpu.VMEM((2, POINTS, LINES, PART), BF16)
    total = POINTS * LINES
    pair = pltpu.SemaphoreType.DMA((2,))
    return pl.pallas_call(
        remap_kernel,
        out_shape=jax.ShapeDtypeStruct((ROWS, WIDTH), BF16),
        in_specs=[pl.BlockSpec(memory_space=pl.ANY)] * 7,
        out_specs=vmem,
        scratch_shapes=[
            pltpu.VMEM((2 * PART, WIDTH), BF16),
            pltpu.VMEM((ROWS, WIDTH), BF16),
            pltpu.VMEM((1, WIDTH), F32),
            pltpu.VMEM((2, POINTS), I32),
            pltpu.VMEM((1, FORMS), I32),
            pltpu.SMEM((1, FORMS), I32),
            pltpu.SMEM((1, FORMS), F32),
            pltpu.VMEM((FREQS * LINES, WIDTH), BF16),
            pltpu.VMEM((POINTS, PART), F32),
            boxes, boxes, boxes, boxes,
            pltpu.VMEM((total, total), BF16),
            pltpu.VMEM((FREQS * LINES, WIDTH), BF16),
            pltpu.VMEM((32, 1024), F32),
            pltpu.VMEM((2, ROWS, 2 * PART), BF16),
            pltpu.VMEM((2, 2, PART, WIDTH), BF16),
            pltpu.VMEM((ROWS, WIDTH), F32),
            pltpu.SemaphoreType.DMA((7,)), pair, pair, pair, pair, pair, pair,
        ],
        compiler_params=pltpu.CompilerParams(
            collective_id=0, has_side_effects=True, vmem_limit_bytes=62 * 1024 * 1024
        ),
        cost_estimate=pl.CostEstimate(flops=10**10, bytes_accessed=10**7, transcendentals=0),
    )(x, vertex, bubble, sb, rs, shift, coef)


def body(vertex, bubble, cross_deriv, send_blocks, recv_slots, freq_shift, proj_coef):
    out = remap(
        cross_deriv[0], vertex[0], bubble, send_blocks[0].T, recv_slots, freq_shift, proj_coef
    )
    return out[None]


def solution(mesh):
    in_specs = (
        P("pts", "rows", None),
        P("pts", None),
        P("pts", "rows", None),
        P("pts", None, None),
        P("pts", None),
        P("pts", None),
        P("pts", None),
    )
    out_specs = P("pts", "rows", None)
    return jax.shard_map(body, mesh=mesh, in_specs=in_specs, out_specs=out_specs, check_vma=False)
```

```python
import functools

import jax
import jax.numpy as jnp
from jax import lax
from jax.experimental import pallas as pl
from jax.experimental.pallas import tpu as pltpu
from jax.sharding import PartitionSpec as P

MESH = pl.DeviceIdType.MESH
F32, BF16, I32 = jnp.float32, jnp.bfloat16, jnp.int32
FORMS, FREQS, POINTS, SIDE = 15, 64, 64, 4
LINES = 16
WIDTH = FORMS * FREQS
ROWS = WIDTH // 2
OUT_BLOCKS = 3
PART = 256


def hops(delta):
    return sum(min(d, SIDE - d) for d in delta)


DELTAS = sorted(
    ((a, b, c) for a in range(SIDE) for b in range(SIDE) for c in range(SIDE) if (a, b, c) != (0, 0, 0)),
    key=lambda d: (-hops(d), d),
)


def iota(shape, dim):
    return lax.broadcasted_iota(I32, shape, dim)


def remap_kernel(
    x_hbm, v_hbm, bub_hbm, sb_hbm, rs_hbm, shift_hbm, coef_hbm, o_ref,
    x_ref, v_ref, bub_ref, sb_ref, rs_ref, shift_ref, coef_ref, perm_ref, table_ref, ta, ra, ub, rb,
    pick_ref, shift_mat, wide_ref, halves, remapped, acc_ref, out_ref,
    load_sem, send_a, recv_a, send_b, recv_b, send_c, recv_c, store_sem,
):
    me = lax.axis_index("pts")
    row = lax.axis_index("rows")
    mz, my, mx = me // (SIDE * SIDE), (me // SIDE) % SIDE, me % SIDE

    def peer(delta):
        dz, dy, dx = delta
        return (((mz + dz) % SIDE) * SIDE + (my + dy) % SIDE) * SIDE + (mx + dx) % SIDE

    loads = [
        pltpu.make_async_copy(src, dst, load_sem.at[i])
        for i, (src, dst) in enumerate((
            (x_hbm, x_ref.at[pl.ds(0, ROWS)]), (sb_hbm, sb_ref), (rs_hbm, rs_ref), (shift_hbm, shift_ref),
            (coef_hbm, coef_ref), (bub_hbm, bub_ref), (v_hbm, v_ref),
        ))
    ]
    for load in loads:
        load.start()

    barrier = pltpu.get_barrier_semaphore()
    for delta in DELTAS:
        pl.semaphore_signal(barrier, inc=1, device_id={"pts": peer(delta)}, device_id_type=MESH)
    pl.semaphore_signal(barrier, inc=1, device_id={"rows": 1 - row}, device_id_type=MESH)

    def build_perm(i, _):
        base = pl.multiple_of(i * 128, 128)
        line = iota((128, 1), 0) + base
        g = line & (LINES - 1)
        want = jnp.where(g < FORMS, g * FREQS + (line >> 4), -1)
        perm_ref[pl.ds(base, 128), :] = jnp.where(want == iota((128, WIDTH), 1), 1.0, 0.0).astype(BF16)
        return 0

    lax.fori_loop(0, FREQS * LINES // 128, build_perm, 0)
    table_ref[...] = jnp.zeros_like(table_ref)
    loads[1].wait()
    loads[2].wait()
    table_ref[0:1, 0:POINTS] = sb_ref[0:1, :].astype(F32)
    table_ref[0:1, POINTS : POINTS + FORMS] = rs_ref[...].astype(F32)
    table_ref[0:1, 128 : 128 + POINTS] = sb_ref[1:2, :].astype(F32)
    x_ref[ROWS:, :] = jnp.zeros((2 * PART - ROWS, WIDTH), BF16)
    loads[0].wait()

    def permute(s):
        block = lax.dot_general(
            perm_ref[...], x_ref[s * PART : (s + 1) * PART, :], (((1,), (1,)), ((), ())),
            preferred_element_type=F32,
        ).reshape(FREQS, LINES, PART)
        if s == 0:
            is_table = iota((FREQS, LINES, PART), 1) == FORMS
            block = jnp.where(is_table, table_ref[0:1, :].reshape(1, 1, PART), block)
        ta[s] = block.astype(BF16)

    permute(0)
    pl.semaphore_wait(barrier, len(DELTAS) + 1)

    def copy_to(src, dst, send, recv, s, p):
        return pltpu.make_async_remote_copy(
            src_ref=src.at[s, p], dst_ref=dst.at[s, me], send_sem=send.at[s], recv_sem=recv.at[s],
            device_id={"pts": p}, device_id_type=MESH,
        )

    def send_all(src, dst, send, recv, s):
        for delta in DELTAS:
            copy_to(src, dst, send, recv, s, peer(delta)).start()
        dst[s, me] = src[s, me]

    def all_of(src, dst, send, recv, s):
        n = len(DELTAS)
        return pltpu.make_async_remote_copy(
            src_ref=src.at[s, pl.ds(0, n)], dst_ref=dst.at[s, pl.ds(0, n)], send_sem=send.at[s],
            recv_sem=recv.at[s], device_id={"pts": peer(DELTAS[0])}, device_id_type=MESH,
        )

    send_all(ta, ra, send_a, recv_a, 0)
    permute(1)
    send_all(ta, ra, send_a, recv_a, 1)

    for load in loads[3:]:
        load.wait()
    wide_ref[:, 896:] = jnp.zeros((32, 128), F32)

    def build_halves(i, _):
        at = pl.ds(pl.multiple_of(i * 32, 32), 32)
        scaled = (v_ref[at, :].astype(F32) * bub_ref[...]).astype(BF16).astype(F32)
        wide_ref[:, :WIDTH] = scaled
        inside = iota((32, 2 * PART), 1) < ROWS
        halves[0, at, :] = jnp.where(inside, wide_ref[:, : 2 * PART], 0.0).astype(BF16)
        halves[1, at, :] = pltpu.roll(wide_ref[...], 1024 - ROWS, 1)[:, : 2 * PART].astype(BF16)
        return 0

    lax.fori_loop(0, ROWS // 32, build_halves, 0)
    lane = iota((1, WIDTH), 1)
    moved_by = jnp.zeros((1, WIDTH), I32)
    weight = jnp.zeros((1, WIDTH), F32)
    for f in range(FORMS):
        here = (lane >> 6) == f
        moved_by = jnp.where(here, shift_ref[0, f], moved_by)
        weight = jnp.where(here, coef_ref[0, f], weight)
    wanted_n = (lane & (FREQS - 1)) + moved_by
    wanted = jnp.where((wanted_n >= 0) & (wanted_n < FREQS), wanted_n * LINES + (lane >> 6), -1)

    def build_shift(i, _):
        base = pl.multiple_of(i * 128, 128)
        line = iota((128, WIDTH), 0) + base
        shift_mat[pl.ds(base, 128), :] = jnp.where(line == wanted, 1.0, 0.0).astype(BF16)
        return 0

    lax.fori_loop(0, FREQS * LINES // 128, build_shift, 0)

    total = POINTS * LINES
    source = iota((POINTS, total), 1)
    widen = jnp.where(iota((POINTS, total), 0) == (source >> 4), 1.0, 0.0).astype(BF16)
    form_of = (source & (LINES - 1)).astype(F32)
    slot_of = ((source >> 4) * 2).astype(F32)

    for s in range(2):
        all_of(ta, ra, send_a, recv_a, s).wait_recv()
        if s == 0:
            tables = ra[0, :, FORMS, :].astype(F32)
            slots = []
            for c in range(2):
                held = lax.dot_general(
                    tables[:, c * 128 : c * 128 + 128].astype(BF16), widen, (((0,), (0,)), ((), ())),
                    preferred_element_type=F32,
                )[:POINTS]
                slots.append(jnp.where(held == form_of, slot_of + c, -7.0))
            table_ref[pl.ds(0, POINTS), 0:128] = tables[:, 0:128]
            for q in range(0, POINTS, 8):
                named = jnp.broadcast_to(
                    table_ref[q : q + 8, 0:128].reshape(8, 1, 128), (8, LINES, 128)
                ).reshape(8 * LINES, 128)
                f = iota((8 * LINES, 128), 0) & (LINES - 1)
                at = iota((8 * LINES, 128), 1)
                named = jnp.sum(jnp.where(at == POINTS + f, named, 0.0), axis=1, keepdims=True)
                named = jnp.where(f[:, 0:1] == FORMS, -1.0, named)
                hit = None
                for c in range(2):
                    slot = jnp.broadcast_to(
                        slots[c][q : q + 8].reshape(8, 1, total), (8, LINES, total)
                    ).reshape(8 * LINES, total)
                    hit = (named == slot) if hit is None else hit | (named == slot)
                pick_ref[q * LINES : (q + 8) * LINES, :] = jnp.where(hit, 1.0, 0.0).astype(BF16)
        for h in range(2):
            chosen = jnp.dot(
                pick_ref[h * total // 2 : (h + 1) * total // 2, :], ra[s].reshape(total, PART),
                preferred_element_type=F32,
            )
            chosen = chosen.astype(BF16).reshape(POINTS // 2, LINES, PART)
            ub[s, h * POINTS // 2 : (h + 1) * POINTS // 2] = chosen
        send_all(ub, rb, send_b, recv_b, s)

    def times(half, s, rows=slice(None)):
        return jnp.dot(
            halves[half, rows, s * PART : (s + 1) * PART], remapped[half, s], preferred_element_type=F32
        )

    swaps, stores = [], []
    for s in range(2):
        all_of(ub, rb, send_b, recv_b, s).wait_recv()
        moved = lax.dot_general(
            rb[s].reshape(FREQS * LINES, PART), shift_mat[...], (((0,), (0,)), ((), ())),
            preferred_element_type=F32,
        )
        remapped[row, s] = (moved * weight).astype(BF16)
        swap = pltpu.make_async_remote_copy(
            src_ref=remapped.at[row, s], dst_ref=remapped.at[row, s], send_sem=send_c.at[s],
            recv_sem=recv_c.at[s], device_id={"rows": 1 - row}, device_id_type=MESH,
        )
        swap.start()
        swaps.append(swap)
        if s == 0:
            acc_ref[...] = times(row, s)
        else:
            acc_ref[...] += times(row, s)
    swaps[0].wait_recv()
    acc_ref[...] += times(1 - row, 0)
    swaps[1].wait_recv()
    step = ROWS // OUT_BLOCKS
    for b in range(OUT_BLOCKS):
        rows = slice(b * step, (b + 1) * step)
        out_ref[rows, :] = (acc_ref[rows, :] + times(1 - row, 1, rows)).astype(BF16)
        at = pl.ds(b * step, step)
        stores.append(pltpu.make_async_copy(out_ref.at[at], o_ref.at[at], store_sem.at[b]))
        stores[-1].start()
    for s in range(2):
        all_of(ta, ra, send_a, recv_a, s).wait_send()
        all_of(ub, rb, send_b, recv_b, s).wait_send()
        swaps[s].wait_send()
    for store in stores:
        store.wait()


def remap(x, vertex, bubble, sb, rs, shift, coef):
    boxes = pltpu.VMEM((2, POINTS, LINES, PART), BF16)
    total = POINTS * LINES
    pair = pltpu.SemaphoreType.DMA((2,))
    return pl.pallas_call(
        remap_kernel,
        out_shape=jax.ShapeDtypeStruct((ROWS, WIDTH), BF16),
        in_specs=[pl.BlockSpec(memory_space=pl.ANY)] * 7,
        out_specs=pl.BlockSpec(memory_space=pl.ANY),
        scratch_shapes=[
            pltpu.VMEM((2 * PART, WIDTH), BF16),
            pltpu.VMEM((ROWS, WIDTH), BF16),
            pltpu.VMEM((1, WIDTH), F32),
            pltpu.VMEM((2, POINTS), I32),
            pltpu.VMEM((1, FORMS), I32),
            pltpu.SMEM((1, FORMS), I32),
            pltpu.SMEM((1, FORMS), F32),
            pltpu.VMEM((FREQS * LINES, WIDTH), BF16),
            pltpu.VMEM((POINTS, PART), F32),
            boxes, boxes, boxes, boxes,
            pltpu.VMEM((total, total), BF16),
            pltpu.VMEM((FREQS * LINES, WIDTH), BF16),
            pltpu.VMEM((32, 1024), F32),
            pltpu.VMEM((2, ROWS, 2 * PART), BF16),
            pltpu.VMEM((2, 2, PART, WIDTH), BF16),
            pltpu.VMEM((ROWS, WIDTH), F32),
            pltpu.VMEM((ROWS, WIDTH), BF16),
            pltpu.SemaphoreType.DMA((7,)), pair, pair, pair, pair, pair, pair,
            pltpu.SemaphoreType.DMA((OUT_BLOCKS,)),
        ],
        compiler_params=pltpu.CompilerParams(
            collective_id=0, has_side_effects=True, vmem_limit_bytes=62 * 1024 * 1024
        ),
        cost_estimate=pl.CostEstimate(flops=10**10, bytes_accessed=10**7, transcendentals=0),
    )(x, vertex, bubble, sb, rs, shift, coef)


def body(vertex, bubble, cross_deriv, send_blocks, recv_slots, freq_shift, proj_coef):
    out = remap(
        cross_deriv[0], vertex[0], bubble, send_blocks[0].T, recv_slots, freq_shift, proj_coef
    )
    return out[None]


def solution(mesh):
    in_specs = (
        P("pts", "rows", None),
        P("pts", None),
        P("pts", "rows", None),
        P("pts", None, None),
        P("pts", None),
        P("pts", None),
        P("pts", None),
    )
    out_specs = P("pts", "rows", None)
    return jax.shard_map(body, mesh=mesh, in_specs=in_specs, out_specs=out_specs, check_vma=False)
```

```python
import functools

import jax
import jax.numpy as jnp
from jax import lax
from jax.experimental import pallas as pl
from jax.experimental.pallas import tpu as pltpu
from jax.sharding import PartitionSpec as P

MESH = pl.DeviceIdType.MESH
F32, BF16, I32 = jnp.float32, jnp.bfloat16, jnp.int32
FORMS, FREQS, POINTS, SIDE = 15, 64, 64, 4
LINES = 16
WIDTH = FORMS * FREQS
ROWS = WIDTH // 2
OUT_BLOCKS = 3
USED = (256, 224)
PART = 256


def hops(delta):
    return sum(min(d, SIDE - d) for d in delta)


DELTAS = sorted(
    ((a, b, c) for a in range(SIDE) for b in range(SIDE) for c in range(SIDE) if (a, b, c) != (0, 0, 0)),
    key=lambda d: (-hops(d), d),
)


def iota(shape, dim):
    return lax.broadcasted_iota(I32, shape, dim)


def remap_kernel(
    x_hbm, v_hbm, bub_hbm, sb_hbm, rs_hbm, shift_hbm, coef_hbm, o_ref,
    x_ref, v_ref, bub_ref, sb_ref, rs_ref, shift_ref, coef_ref, perm_ref, table_ref, ta, ra, ub, rb,
    pick_ref, shift_mat, wide_ref, halves, remapped, acc_ref, out_ref,
    load_sem, send_a, recv_a, send_b, recv_b, send_c, recv_c, store_sem,
):
    me = lax.axis_index("pts")
    row = lax.axis_index("rows")
    mz, my, mx = me // (SIDE * SIDE), (me // SIDE) % SIDE, me % SIDE

    def peer(delta):
        dz, dy, dx = delta
        return (((mz + dz) % SIDE) * SIDE + (my + dy) % SIDE) * SIDE + (mx + dx) % SIDE

    loads = [
        pltpu.make_async_copy(src, dst, load_sem.at[i])
        for i, (src, dst) in enumerate((
            (x_hbm, x_ref.at[pl.ds(0, ROWS)]), (sb_hbm, sb_ref), (rs_hbm, rs_ref), (shift_hbm, shift_ref),
            (coef_hbm, coef_ref), (bub_hbm, bub_ref), (v_hbm, v_ref),
        ))
    ]
    for load in loads:
        load.start()

    barrier = pltpu.get_barrier_semaphore()
    for delta in DELTAS:
        pl.semaphore_signal(barrier, inc=1, device_id={"pts": peer(delta)}, device_id_type=MESH)
    pl.semaphore_signal(barrier, inc=1, device_id={"rows": 1 - row}, device_id_type=MESH)

    def build_perm(i, _):
        base = pl.multiple_of(i * 128, 128)
        line = iota((128, 1), 0) + base
        g = line & (LINES - 1)
        want = jnp.where(g < FORMS, g * FREQS + (line >> 4), -1)
        perm_ref[pl.ds(base, 128), :] = jnp.where(want == iota((128, WIDTH), 1), 1.0, 0.0).astype(BF16)
        return 0

    lax.fori_loop(0, FREQS * LINES // 128, build_perm, 0)
    table_ref[...] = jnp.zeros_like(table_ref)
    loads[1].wait()
    loads[2].wait()
    table_ref[0:1, 0:POINTS] = sb_ref[0:1, :].astype(F32)
    table_ref[0:1, POINTS : POINTS + FORMS] = rs_ref[...].astype(F32)
    table_ref[0:1, 128 : 128 + POINTS] = sb_ref[1:2, :].astype(F32)
    x_ref[ROWS:, :] = jnp.zeros((2 * PART - ROWS, WIDTH), BF16)
    loads[0].wait()

    def permute(s):
        block = lax.dot_general(
            perm_ref[...], x_ref[s * PART : (s + 1) * PART, :], (((1,), (1,)), ((), ())),
            preferred_element_type=F32,
        ).reshape(FREQS, LINES, PART)
        if s == 0:
            is_table = iota((FREQS, LINES, PART), 1) == FORMS
            block = jnp.where(is_table, table_ref[0:1, :].reshape(1, 1, PART), block)
        ta[s] = block.astype(BF16)

    permute(0)
    pl.semaphore_wait(barrier, len(DELTAS) + 1)

    def copy_to(src, dst, send, recv, s, p):
        return pltpu.make_async_remote_copy(
            src_ref=src.at[s, p], dst_ref=dst.at[s, me], send_sem=send.at[s], recv_sem=recv.at[s],
            device_id={"pts": p}, device_id_type=MESH,
        )

    def send_all(src, dst, send, recv, s):
        for delta in DELTAS:
            copy_to(src, dst, send, recv, s, peer(delta)).start()
        dst[s, me] = src[s, me]

    def all_of(src, dst, send, recv, s):
        n = len(DELTAS)
        return pltpu.make_async_remote_copy(
            src_ref=src.at[s, pl.ds(0, n)], dst_ref=dst.at[s, pl.ds(0, n)], send_sem=send.at[s],
            recv_sem=recv.at[s], device_id={"pts": peer(DELTAS[0])}, device_id_type=MESH,
        )

    send_all(ta, ra, send_a, recv_a, 0)
    permute(1)
    send_all(ta, ra, send_a, recv_a, 1)

    for load in loads[3:]:
        load.wait()
    wide_ref[:, 896:] = jnp.zeros((32, 128), F32)

    def build_halves(i, _):
        at = pl.ds(pl.multiple_of(i * 32, 32), 32)
        scaled = (v_ref[at, :].astype(F32) * bub_ref[...]).astype(BF16).astype(F32)
        wide_ref[:, :WIDTH] = scaled
        inside = iota((32, 2 * PART), 1) < ROWS
        halves[0, at, :] = jnp.where(inside, wide_ref[:, : 2 * PART], 0.0).astype(BF16)
        halves[1, at, :] = pltpu.roll(wide_ref[...], 1024 - ROWS, 1)[:, : 2 * PART].astype(BF16)
        return 0

    lax.fori_loop(0, ROWS // 32, build_halves, 0)
    lane = iota((1, WIDTH), 1)
    moved_by = jnp.zeros((1, WIDTH), I32)
    weight = jnp.zeros((1, WIDTH), F32)
    for f in range(FORMS):
        here = (lane >> 6) == f
        moved_by = jnp.where(here, shift_ref[0, f], moved_by)
        weight = jnp.where(here, coef_ref[0, f], weight)
    wanted_n = (lane & (FREQS - 1)) + moved_by
    wanted = jnp.where((wanted_n >= 0) & (wanted_n < FREQS), wanted_n * LINES + (lane >> 6), -1)

    def build_shift(i, _):
        base = pl.multiple_of(i * 128, 128)
        line = iota((128, WIDTH), 0) + base
        shift_mat[pl.ds(base, 128), :] = jnp.where(line == wanted, 1.0, 0.0).astype(BF16)
        return 0

    lax.fori_loop(0, FREQS * LINES // 128, build_shift, 0)

    total = POINTS * LINES
    source = iota((POINTS, total), 1)
    widen = jnp.where(iota((POINTS, total), 0) == (source >> 4), 1.0, 0.0).astype(BF16)
    form_of = (source & (LINES - 1)).astype(F32)
    slot_of = ((source >> 4) * 2).astype(F32)

    for s in range(2):
        all_of(ta, ra, send_a, recv_a, s).wait_recv()
        if s == 0:
            tables = ra[0, :, FORMS, :].astype(F32)
            slots = []
            for c in range(2):
                held = lax.dot_general(
                    tables[:, c * 128 : c * 128 + 128].astype(BF16), widen, (((0,), (0,)), ((), ())),
                    preferred_element_type=F32,
                )[:POINTS]
                slots.append(jnp.where(held == form_of, slot_of + c, -7.0))
            table_ref[pl.ds(0, POINTS), 0:128] = tables[:, 0:128]
            for q in range(0, POINTS, 8):
                named = jnp.broadcast_to(
                    table_ref[q : q + 8, 0:128].reshape(8, 1, 128), (8, LINES, 128)
                ).reshape(8 * LINES, 128)
                f = iota((8 * LINES, 128), 0) & (LINES - 1)
                at = iota((8 * LINES, 128), 1)
                named = jnp.sum(jnp.where(at == POINTS + f, named, 0.0), axis=1, keepdims=True)
                named = jnp.where(f[:, 0:1] == FORMS, -1.0, named)
                hit = None
                for c in range(2):
                    slot = jnp.broadcast_to(
                        slots[c][q : q + 8].reshape(8, 1, total), (8, LINES, total)
                    ).reshape(8 * LINES, total)
                    hit = (named == slot) if hit is None else hit | (named == slot)
                pick_ref[q * LINES : (q + 8) * LINES, :] = jnp.where(hit, 1.0, 0.0).astype(BF16)
        for h in range(2):
            chosen = jnp.dot(
                pick_ref[h * total // 2 : (h + 1) * total // 2, :], ra[s].reshape(total, PART),
                preferred_element_type=F32,
            )
            chosen = chosen.astype(BF16).reshape(POINTS // 2, LINES, PART)
            ub[s, h * POINTS // 2 : (h + 1) * POINTS // 2] = chosen
        send_all(ub, rb, send_b, recv_b, s)

    def times(half, s, rows=slice(None)):
        return jnp.dot(
            halves[half, rows, s * PART : s * PART + USED[s]], remapped[half, s, : USED[s]],
            preferred_element_type=F32,
        )

    swaps, stores = [], []
    for s in range(2):
        all_of(ub, rb, send_b, recv_b, s).wait_recv()
        moved = lax.dot_general(
            rb[s].reshape(FREQS * LINES, PART), shift_mat[...], (((0,), (0,)), ((), ())),
            preferred_element_type=F32,
        )
        remapped[row, s, : USED[s]] = (moved * weight).astype(BF16)[: USED[s]]
        where = remapped.at[row, s, pl.ds(0, USED[s])]
        swap = pltpu.make_async_remote_copy(
            src_ref=where, dst_ref=where, send_sem=send_c.at[s],
            recv_sem=recv_c.at[s], device_id={"rows": 1 - row}, device_id_type=MESH,
        )
        swap.start()
        swaps.append(swap)
        if s == 0:
            acc_ref[...] = times(row, s)
        else:
            acc_ref[...] += times(row, s)
    swaps[0].wait_recv()
    acc_ref[...] += times(1 - row, 0)
    swaps[1].wait_recv()
    step = ROWS // OUT_BLOCKS
    for b in range(OUT_BLOCKS):
        rows = slice(b * step, (b + 1) * step)
        out_ref[rows, :] = (acc_ref[rows, :] + times(1 - row, 1, rows)).astype(BF16)
        at = pl.ds(b * step, step)
        stores.append(pltpu.make_async_copy(out_ref.at[at], o_ref.at[at], store_sem.at[b]))
        stores[-1].start()
    for s in range(2):
        all_of(ta, ra, send_a, recv_a, s).wait_send()
        all_of(ub, rb, send_b, recv_b, s).wait_send()
        swaps[s].wait_send()
    for store in stores:
        store.wait()


def remap(x, vertex, bubble, sb, rs, shift, coef):
    boxes = pltpu.VMEM((2, POINTS, LINES, PART), BF16)
    total = POINTS * LINES
    pair = pltpu.SemaphoreType.DMA((2,))
    return pl.pallas_call(
        remap_kernel,
        out_shape=jax.ShapeDtypeStruct((ROWS, WIDTH), BF16),
        in_specs=[pl.BlockSpec(memory_space=pl.ANY)] * 7,
        out_specs=pl.BlockSpec(memory_space=pl.ANY),
        scratch_shapes=[
            pltpu.VMEM((2 * PART, WIDTH), BF16),
            pltpu.VMEM((ROWS, WIDTH), BF16),
            pltpu.VMEM((1, WIDTH), F32),
            pltpu.VMEM((2, POINTS), I32),
            pltpu.VMEM((1, FORMS), I32),
            pltpu.SMEM((1, FORMS), I32),
            pltpu.SMEM((1, FORMS), F32),
            pltpu.VMEM((FREQS * LINES, WIDTH), BF16),
            pltpu.VMEM((POINTS, PART), F32),
            boxes, boxes, boxes, boxes,
            pltpu.VMEM((total, total), BF16),
            pltpu.VMEM((FREQS * LINES, WIDTH), BF16),
            pltpu.VMEM((32, 1024), F32),
            pltpu.VMEM((2, ROWS, 2 * PART), BF16),
            pltpu.VMEM((2, 2, PART, WIDTH), BF16),
            pltpu.VMEM((ROWS, WIDTH), F32),
            pltpu.VMEM((ROWS, WIDTH), BF16),
            pltpu.SemaphoreType.DMA((7,)), pair, pair, pair, pair, pair, pair,
            pltpu.SemaphoreType.DMA((OUT_BLOCKS,)),
        ],
        compiler_params=pltpu.CompilerParams(
            collective_id=0, has_side_effects=True, vmem_limit_bytes=62 * 1024 * 1024
        ),
        cost_estimate=pl.CostEstimate(flops=10**10, bytes_accessed=10**7, transcendentals=0),
    )(x, vertex, bubble, sb, rs, shift, coef)


def body(vertex, bubble, cross_deriv, send_blocks, recv_slots, freq_shift, proj_coef):
    out = remap(
        cross_deriv[0], vertex[0], bubble, send_blocks[0].T, recv_slots, freq_shift, proj_coef
    )
    return out[None]


def solution(mesh):
    in_specs = (
        P("pts", "rows", None),
        P("pts", None),
        P("pts", "rows", None),
        P("pts", None, None),
        P("pts", None),
        P("pts", None),
        P("pts", None),
    )
    out_specs = P("pts", "rows", None)
    return jax.shard_map(body, mesh=mesh, in_specs=in_specs, out_specs=out_specs, check_vma=False)
```
